32 devices in a mesh: section: 2 (over core), mp: 4 (over y, x), dp: 4 (over z).
Axes of the slice: x: 2, y: 2, z: 4, core: 2. Of those that a mesh axis runs over, the one named last changes fastest.
Arguments:
- value_grad: bfloat16 [2, 2048, 3072], P('section', 'dp', 'mp'), may hold values from -6 to 6
- stream: bfloat16 [2, 2048, 3072], P('section', 'dp'), may hold values from -300 to 300
- weights: bfloat16 [2, 3072, 3072], P('section', 'mp'), may hold values from -0.109375 to 0.109375
- gain: float32 [2, 3072], P('section'), may hold values from 0.25 to 1.75
- top_grad: bfloat16 [2048, 3072], P('dp'), may hold values from -6 to 6
- counts: int32 [4], P('dp'), may hold values from 1 to 2, as said below
Outputs:
- weight_grad: bfloat16 [2, 3072, 3072], P('section', ('mp', 'dp'))
- residual_grad: bfloat16 [2, 2048, 3072], P('section', 'dp', 'mp')
The draws below stay inside these ranges and needn't reach their ends.
Inputs may be any that keep to these rules, and one draw needn't show every extreme that they name: counts[r] counts the live micro-batches of replica r; some replica has all 2.
All inputs are finite; a program needn't handle non-finite values.
Results may differ from the reference program's by a relative error of at most 0.009.
Values may be sent and summed in bfloat16 or wider, within the bound.
A program may use at most 64 MiB of HBM per device.

```python
import jax
import jax.numpy as jnp
from jax import lax

D = 3072
F = 3072
MICRO = 2
TOK_MB = 256
GROUPS = 4
REPLICAS = 4
TOKENS = 2048


def draw_stream(key, part):
    first, second, third = jax.random.split(key, 3)
    row_scale = jnp.exp(jax.random.uniform(second, (2, TOKENS, 1), jnp.float32) * jnp.log(10.0))
    col_scale = jnp.exp(jax.random.uniform(third, (2, 1, D), jnp.float32) * jnp.log(10.0))
    base = jax.random.normal(first, (2, TOKENS, D), jnp.float32)
    values = jnp.clip(base * row_scale * col_scale * 0.3, -300.0, 300.0)
    return values.astype(jnp.bfloat16)


def draw_counts(key, part):
    first, second = jax.random.split(jax.random.fold_in(key, 7))
    drawn = jax.random.randint(first, (REPLICAS,), 1, MICRO + 1)
    chosen = jax.random.randint(second, (), 0, REPLICAS)
    drawn = drawn.at[chosen].set(MICRO)
    return drawn.astype(jnp.int32)


def strengthened(entries, rng, source, target, shards_of, factor):
    def block_of(position):
        return (jnp.arange(entries.shape[position]) // (entries.shape[position] // shards_of)).reshape((-1,) + (1,) * (entries.ndim - 1 - position))

    near = jax.random.permutation(rng, shards_of)[block_of(target)]
    second = (block_of(target) + shards_of // 2) % shards_of
    return jnp.where((block_of(source) == near) | (block_of(source) == second), factor * entries, entries)


def shard_levels(own_key, extent, shards, least, top_value):
    def one(position, shards_of):
        steps = jax.random.uniform(jax.random.fold_in(jax.random.fold_in(own_key, 6), position), (shards_of,), jnp.float32, least / len(shards), top_value / len(shards))
        return jnp.repeat(jnp.exp(steps), extent[position] // shards_of).reshape((-1,) + (1,) * (len(extent) - position - 1))

    loudness = one(*shards[0])
    for cut in shards[1:]:
        loudness = loudness * one(*cut)
    return loudness


def noise(rng, dims, deviation, reach, shards=(), kind=jnp.bfloat16):
    array = jax.random.normal(rng, dims, jnp.float32) * deviation
    if len(shards) > 0:
        array = shard_levels(rng, dims, shards, -0.22, 0.18) * array
    return jnp.clip(array, min=-reach, max=reach).astype(kind)


def gaussian_with(stream_key, shape, scale, bound, cuts, heavy, kind=jnp.bfloat16):
    entries = scale * jax.random.normal(stream_key, shape, jnp.float32)
    if cuts:
        entries = entries * shard_levels(stream_key, shape, cuts, -0.22, 0.18)
    return jnp.clip(strengthened(entries, jax.random.fold_in(stream_key, 3), *heavy), -bound, bound).astype(kind)


def setup_inputs(seed: int = 0) -> dict:
    seeds = jax.random.split(jax.random.key(seed), 7)
    value_grad = gaussian_with(seeds[0], (2, TOKENS, F), 1.0, 6.0, ((0, 2), (1, 4), (2, 4)), (1, 2, 4, 2.0))
    stream = draw_stream(jax.random.fold_in(seeds[6], 71), 0)
    weights = noise(seeds[2], (2, F, D), D ** -0.5, 0.109375, ((0, 2), (1, 4)))
    gain = jnp.clip(1.0 + 0.15 * jax.random.normal(seeds[3], (2, D), jnp.float32), 0.25, 1.75)
    top_grad = noise(seeds[4], (TOKENS, D), 1.0, 6.0, ((0, 4),))
    counts = draw_counts(jax.random.fold_in(seeds[6], 71), 0)
    return {"value_grad": value_grad, "stream": stream, "weights": weights, "gain": gain, "top_grad": top_grad, "counts": counts}


def normalize(stream_rows):
    values = stream_rows.astype(jnp.float32)
    average = lax.optimization_barrier(jnp.mean(values, axis=-1, keepdims=True))
    centred = values - average
    variance = lax.optimization_barrier(jnp.mean(centred * centred, axis=-1, keepdims=True))
    inv_scale = lax.rsqrt(variance + 1e-06)
    return (centred * inv_scale, inv_scale)

def reference(value_grad, stream, weights, gain, top_grad, counts):
    per_replica = MICRO * TOK_MB
    token_index = jnp.arange(TOKENS, dtype=jnp.int32)
    replica = token_index // per_replica
    micro_index = token_index % per_replica // TOK_MB
    live_mask = (micro_index < counts[replica]).astype(jnp.bfloat16)
    block_rows = F // GROUPS
    weight_grads = []
    branch_terms = []
    for section_index in range(2):
        whitened, inv_scale = normalize(stream[section_index])
        gain_row = gain[section_index].astype(jnp.float32)
        normed = (whitened * gain_row).astype(jnp.bfloat16)
        masked = value_grad[section_index] * live_mask[:, None]
        weight_grads.append(jnp.dot(masked.T, normed, preferred_element_type=jnp.float32).astype(jnp.bfloat16))
        norm_grad = jnp.zeros((TOKENS, D), jnp.float32)
        for block_index in range(GROUPS):
            low = block_index * block_rows
            partial_value = jnp.dot(value_grad[section_index][:, low:low + block_rows], weights[section_index][low:low + block_rows], preferred_element_type=jnp.float32).astype(jnp.bfloat16)
            norm_grad = norm_grad + lax.optimization_barrier(partial_value).astype(jnp.float32)
        scaled_grad = norm_grad * gain_row
        first_mean = lax.optimization_barrier(jnp.mean(scaled_grad, axis=-1, keepdims=True))
        second_mean = lax.optimization_barrier(jnp.mean(scaled_grad * whitened, axis=-1, keepdims=True))
        branch_terms.append(inv_scale * (scaled_grad - first_mean - whitened * second_mean))
    above_grad = (top_grad.astype(jnp.float32) + branch_terms[1]).astype(jnp.bfloat16)
    lower_grad = (above_grad.astype(jnp.float32) + branch_terms[0]).astype(jnp.bfloat16)
    return (jnp.stack(weight_grads), jnp.stack([lower_grad, above_grad]))
```

```python
import jax
import jax.numpy as jnp
from jax import lax
from jax.sharding import PartitionSpec as P

TOK_MB = 256


def normalize(stream_rows):
    values = stream_rows.astype(jnp.float32)
    average = jnp.mean(values, axis=-1, keepdims=True)
    centred = values - average
    variance = jnp.mean(centred * centred, axis=-1, keepdims=True)
    inv_scale = lax.rsqrt(variance + 1e-06)
    return (centred * inv_scale, inv_scale)


def shards(value_grad, stream, weights, gain, top_grad, counts):
    section_index = lax.axis_index("section")
    model_index = lax.axis_index("mp")
    row_total = stream.shape[1]
    whitened, inv_scale = normalize(stream[0])
    gain_row = gain[0]
    width = whitened.shape[1]
    share = width // lax.axis_size("mp")
    first_col = model_index * share
    cols = lambda a: lax.dynamic_slice_in_dim(a, first_col, share, 1)
    partial = jnp.dot(value_grad[0], weights[0], preferred_element_type=jnp.float32)
    partial = partial.astype(jnp.bfloat16)
    local = partial.astype(jnp.float32) * gain_row
    sums = jnp.stack([jnp.sum(local, -1), jnp.sum(local * whitened, -1)])
    norm_grad = lax.psum_scatter(partial, "mp", scatter_dimension=1, tiled=True)
    sums = lax.psum(sums, "mp") * (1.0 / width)
    normed = (whitened * gain_row).astype(jnp.bfloat16)
    micro_index = jnp.arange(row_total, dtype=jnp.int32) // TOK_MB
    live_mask = (micro_index < counts[0]).astype(jnp.bfloat16)
    masked = value_grad[0] * live_mask[:, None]
    product = lax.dot_general(
        masked, normed, (((0,), (0,)), ((), ())), preferred_element_type=jnp.float32
    )
    weight_grad = lax.psum_scatter(
        product.astype(jnp.bfloat16), "dp", scatter_dimension=0, tiled=True
    )[None]
    scaled = norm_grad.astype(jnp.float32) * cols(gain)
    branch = inv_scale * (scaled - sums[0][:, None] - cols(whitened) * sums[1][:, None])
    above = (cols(top_grad).astype(jnp.float32) + branch).astype(jnp.bfloat16)
    below = lax.ppermute(above, "section", [(1, 0)])
    lower = (below.astype(jnp.float32) + branch).astype(jnp.bfloat16)
    result = jnp.where(section_index == 0, lower, above)
    return (weight_grad, result[None])


def solution(mesh):
    in_specs = (
        P("section", "dp", "mp"),
        P("section", "dp", None),
        P("section", "mp", None),
        P("section", None),
        P("dp", None),
        P("dp"),
    )
    out_specs = (P("section", ("mp", "dp"), None), P("section", "dp", "mp"))
    return jax.shard_map(shards, mesh=mesh, in_specs=in_specs, out_specs=out_specs, check_vma=False)
```

```python
import functools

import jax
import jax.numpy as jnp
from jax import lax
from jax.experimental import pallas as pl
from jax.experimental.pallas import tpu as pltpu
from jax.sharding import PartitionSpec as P

MESH = pl.DeviceIdType.MESH
TOK_MB = 256
CHUNK = 512
F32, BF16 = jnp.float32, jnp.bfloat16


def kernel(
    n, m, vgt, vg, x, w_hbm, gain, top_hbm, wg, res,
    w, top, normed, stats, own, from_left, from_right, psend, precv, acc1, acc2, ssend, srecv, above, below,
    local_sem, right_send, right_recv, left_send, left_recv, p_send, p_recv, s_send, s_recv, sec_send, sec_recv,
):
    sec, me, r = lax.axis_index("section"), lax.axis_index("mp"), lax.axis_index("dp")
    tokens, width = x.shape
    share = width // m
    chunks = width // CHUNK
    rows_mp = min(128, tokens)
    my_cols = pl.ds(pl.multiple_of(me * share, 128), share)

    load_w = pltpu.make_async_copy(w_hbm, w, local_sem.at[0])
    load_top = pltpu.make_async_copy(top_hbm.at[:, my_cols], top, local_sem.at[1])
    load_w.start()
    load_top.start()

    barrier = pltpu.get_barrier_semaphore()
    for k in range(1, m):
        pl.semaphore_signal(barrier, inc=1, device_id={"mp": lax.rem(me + k, m)}, device_id_type=MESH)
    pl.semaphore_signal(barrier, inc=1, device_id={"section": 1 - sec}, device_id_type=MESH)

    @pl.when(r > 0)
    def _():
        pl.semaphore_signal(barrier, inc=1, device_id={"dp": r - 1}, device_id_type=MESH)

    @pl.when(r < n - 1)
    def _():
        pl.semaphore_signal(barrier, inc=1, device_id={"dp": r + 1}, device_id_type=MESH)

    lane = lambda rows: lax.broadcasted_iota(jnp.int32, (rows, 128), 1)

    def norm_tile(i, _):
        rows = pl.ds(pl.multiple_of(i * 16, 16), 16)
        values = x[rows, :].astype(F32)
        average = jnp.sum(values, axis=-1, keepdims=True) * (1.0 / width)
        centred = values - average
        variance = jnp.sum(centred * centred, axis=-1, keepdims=True) * (1.0 / width)
        inv = lax.rsqrt(variance + 1e-06)
        normed[rows, :] = (centred * inv * gain[...]).astype(BF16)
        stats[rows, :] = jnp.where(lane(16) == 0, average, inv)
        return 0

    lax.fori_loop(0, tokens // 16, norm_tile, 0)

    pl.semaphore_wait(barrier, m + jnp.where(r > 0, 1, 0) + jnp.where(r < n - 1, 1, 0))

    def right_copy(c, b, source):
        return pltpu.make_async_remote_copy(
            src_ref=source.at[c, b], dst_ref=from_left.at[c, b], send_sem=right_send.at[c, b],
            recv_sem=right_recv.at[c, b], device_id={"dp": lax.rem(r + 1, n)}, device_id_type=MESH,
        )

    def left_copy(c, b, source):
        return pltpu.make_async_remote_copy(
            src_ref=source.at[c, b], dst_ref=from_right.at[c, b], send_sem=left_send.at[c, b],
            recv_sem=left_recv.at[c, b], device_id={"dp": lax.rem(r + n - 1, n)}, device_id_type=MESH,
        )

    def product(c):
        def block(i, _):
            b = jnp.where(r == 0, n - 1 - i, i)
            own[c, b] = jnp.dot(
                vgt[b], normed[:, c * CHUNK:(c + 1) * CHUNK], preferred_element_type=F32
            ).astype(BF16)

            @pl.when((r == 0) & (b > 0))
            def _():
                right_copy(c, b, own).start()

            @pl.when((r == n - 1) & (b < n - 1))
            def _():
                left_copy(c, b, own).start()

            return 0

        lax.fori_loop(0, n, block, 0)

    def peer(k):
        return {"mp": lax.rem(me + k, m)}

    def part_copy(k):
        return pltpu.make_async_remote_copy(
            src_ref=psend.at[k], dst_ref=precv.at[k], send_sem=p_send.at[k], recv_sem=p_recv.at[k],
            device_id=peer(k), device_id_type=MESH,
        )

    def sum_copy(k):
        return pltpu.make_async_remote_copy(
            src_ref=ssend, dst_ref=srecv.at[k], send_sem=s_send.at[k], recv_sem=s_recv.at[k],
            device_id=peer(k), device_id_type=MESH,
        )

    def fold(value):
        total = value[:, :128]
        for start in range(128, value.shape[1], 128):
            total = total + value[:, start:start + 128]
        return total

    def whitened_of(rows, cols):
        return (x[rows, cols].astype(F32) - stats[rows, 0:1]) * stats[rows, 1:2]

    def partials():
        load_w.wait()
        for step in range(m):
            k = (step + 1) % m
            cols = pl.ds(pl.multiple_of(lax.rem(me + k, m) * share, 128), share)

            def tile(i, _):
                rows = pl.ds(pl.multiple_of(i * rows_mp, rows_mp), rows_mp)
                part = jnp.dot(vg[rows, :], w[:, cols], preferred_element_type=F32)
                psend[k, rows, :] = part.astype(BF16)
                scaled = part * gain[:, cols]
                first, second = fold(scaled), fold(scaled * whitened_of(rows, cols))
                if step == 0:
                    acc1[rows, :] = first
                    acc2[rows, :] = second
                elif step < m - 1:
                    acc1[rows, :] += first
                    acc2[rows, :] += second
                else:
                    one = jnp.sum(acc1[rows, :] + first, axis=-1, keepdims=True)
                    two = jnp.sum(acc2[rows, :] + second, axis=-1, keepdims=True)
                    ssend[rows, :] = jnp.where(lane(rows_mp) == 0, one, two)
                return 0

            lax.fori_loop(0, tokens // rows_mp, tile, 0)
            if k > 0:
                part_copy(k).start()
        for k in range(1, m):
            sum_copy(k).start()

    def section_copy():
        return pltpu.make_async_remote_copy(
            src_ref=above, dst_ref=below, send_sem=sec_send, recv_sem=sec_recv,
            device_id={"section": 1 - sec}, device_id_type=MESH,
        )

    def residual(base, extra):
        def tile(i, _):
            rows = pl.ds(pl.multiple_of(i * 64, 64), 64)
            grad = psend[0, rows, :].astype(F32)
            sums = ssend[rows, :]
            for k in range(1, m):
                grad = grad + precv[k, rows, :].astype(F32)
                sums = sums + srecv[k, rows, :]
            sums = sums * (1.0 / width)
            scaled = grad * gain[:, my_cols]
            white = whitened_of(rows, my_cols)
            branch = stats[rows, 1:2] * (scaled - sums[:, 0:1] - white * sums[:, 1:2])
            value = (base[rows, :].astype(F32) + branch).astype(BF16)
            res[rows, :] = value
            if extra is not None:
                extra[rows, :] = value
            return 0

        lax.fori_loop(0, tokens // 64, tile, 0)

    def finish_later():
        load_top.wait()
        for k in range(1, m):
            part_copy(k).wait_recv()
            sum_copy(k).wait_recv()

        @pl.when(sec == 1)
        def _():
            residual(top, above)
            section_copy().start()

    def finish_earlier():
        @pl.when(sec == 0)
        def _():
            section_copy().wait_recv()
            residual(below, None)

    def forward(c):
        middle = (r > 0) & (r < n - 1)

        def go_right(i, _):
            b = n - 1 - i
            right_copy(c, b, from_left).wait_recv()
            from_left[c, b] = (from_left[c, b].astype(F32) + own[c, b].astype(F32)).astype(BF16)
            right_copy(c, b, from_left).start()
            return 0

        def go_left(b, _):
            left_copy(c, b, from_right).wait_recv()
            from_right[c, b] = (from_right[c, b].astype(F32) + own[c, b].astype(F32)).astype(BF16)
            left_copy(c, b, from_right).start()
            return 0

        def both(right_first):
            steps = [
                lambda: lax.fori_loop(0, n - 1 - r, go_right, 0),
                lambda: lax.fori_loop(0, r, go_left, 0),
            ]
            for step in steps if right_first else steps[::-1]:
                step()

        @pl.when(middle & (r < n // 2))
        def _():
            both(True)

        @pl.when(middle & (r >= n // 2))
        def _():
            both(False)

    def settle(c):
        cols = slice(c * CHUNK, (c + 1) * CHUNK)

        @pl.when(r == 0)
        def _():
            left_copy(c, r, own).wait_recv()
            wg[:, cols] = (own[c, r].astype(F32) + from_right[c, r].astype(F32)).astype(BF16)

        @pl.when(r == n - 1)
        def _():
            right_copy(c, r, own).wait_recv()
            wg[:, cols] = (own[c, r].astype(F32) + from_left[c, r].astype(F32)).astype(BF16)

        @pl.when((r > 0) & (r < n - 1))
        def _():
            left_copy(c, r, own).wait_recv()
            right_copy(c, r, own).wait_recv()
            wg[:, cols] = (
                own[c, r].astype(F32) + from_left[c, r].astype(F32) + from_right[c, r].astype(F32)
            ).astype(BF16)

    product(0)
    partials()
    for c in range(1, chunks):
        product(c)
    later, earlier = max(chunks - 3, 0), max(chunks - 2, 0)
    for c in range(chunks):
        forward(c)
        settle(c)
        if c == later:
            finish_later()
        if c == earlier:
            finish_earlier()

    for k in range(1, m):
        part_copy(k).wait_send()
        sum_copy(k).wait_send()

    @pl.when(sec == 1)
    def _():
        section_copy().wait_send()

    for c in range(chunks):
        def sent_right(b, _):
            right_copy(c, b, own).wait_send()
            return 0

        def sent_left(b, _):
            left_copy(c, b, own).wait_send()
            return 0

        lax.fori_loop(r + 1, n, sent_right, 0)
        lax.fori_loop(0, r, sent_left, 0)


def solution(mesh):
    n, m = mesh.shape["dp"], mesh.shape["mp"]

    def step(value_grad, stream, weights, gain, top_grad, counts):
        tokens, features = value_grad.shape[1:]
        width = stream.shape[2]
        share, block, chunks = width // m, features // n, width // CHUNK
        micro = jnp.arange(tokens, dtype=jnp.int32) // TOK_MB
        live = (micro < counts[0]).astype(BF16)
        turned = (value_grad[0] * live[:, None]).T.reshape(n, block, tokens)
        vmem = pl.BlockSpec(memory_space=pltpu.VMEM)
        hbm = pl.BlockSpec(memory_space=pl.ANY)
        dma = pltpu.SemaphoreType.DMA
        chain = (chunks, n, block, CHUNK)
        wg, res = pl.pallas_call(
            functools.partial(kernel, n, m),
            out_shape=(
                jax.ShapeDtypeStruct((block, width), BF16),
                jax.ShapeDtypeStruct((tokens, share), BF16),
            ),
            in_specs=[vmem, vmem, vmem, hbm, vmem, hbm],
            out_specs=(vmem, vmem),
            scratch_shapes=[
                pltpu.VMEM((features, width), BF16),
                pltpu.VMEM((tokens, share), BF16),
                pltpu.VMEM((tokens, width), BF16),
                pltpu.VMEM((tokens, 128), F32),
                pltpu.VMEM(chain, BF16),
                pltpu.VMEM(chain, BF16),
                pltpu.VMEM(chain, BF16),
                pltpu.VMEM((m, tokens, share), BF16),
                pltpu.VMEM((m, tokens, share), BF16),
                pltpu.VMEM((tokens, 128), F32),
                pltpu.VMEM((tokens, 128), F32),
                pltpu.VMEM((tokens, 128), F32),
                pltpu.VMEM((m, tokens, 128), F32),
                pltpu.VMEM((tokens, share), BF16),
                pltpu.VMEM((tokens, share), BF16),
                dma((2,)),
                dma((chunks, n)), dma((chunks, n)), dma((chunks, n)), dma((chunks, n)),
                dma((m,)), dma((m,)), dma((m,)), dma((m,)),
                dma, dma,
            ],
            compiler_params=pltpu.CompilerParams(
                collective_id=0, has_side_effects=True, vmem_limit_bytes=56 * 2**20
            ),
        )(turned, value_grad[0], stream[0], weights[0], gain, top_grad)
        return wg[None], res[None]

    in_specs = (
        P("section", "dp", "mp"),
        P("section", "dp", None),
        P("section", "mp", None),
        P("section", None),
        P("dp", None),
        P("dp"),
    )
    out_specs = (P("section", ("mp", "dp"), None), P("section", "dp", "mp"))
    return jax.shard_map(step, mesh=mesh, in_specs=in_specs, out_specs=out_specs, check_vma=False)
```

```python
import functools

import jax
import jax.numpy as jnp
from jax import lax
from jax.experimental import pallas as pl
from jax.experimental.pallas import tpu as pltpu
from jax.sharding import PartitionSpec as P

MESH = pl.DeviceIdType.MESH
TOK_MB = 256
CHUNK = 512
F32, BF16 = jnp.float32, jnp.bfloat16


def kernel(
    n, m, live, vg, x, w_hbm, gain, top_hbm, wg, res,
    w, top, vgt, normed, stats, own, from_left, from_right, psend, precv, acc1, acc2, ssend, srecv, above, below,
    local_sem, right_send, right_recv, left_send, left_recv, p_send, p_recv, s_send, s_recv, sec_send, sec_recv,
):
    sec, me, r = lax.axis_index("section"), lax.axis_index("mp"), lax.axis_index("dp")
    tokens, width = x.shape
    share = width // m
    chunks = width // CHUNK
    rows_mp = min(128, tokens)
    my_cols = pl.ds(pl.multiple_of(me * share, 128), share)

    load_w = pltpu.make_async_copy(w_hbm, w, local_sem.at[0])
    load_top = pltpu.make_async_copy(top_hbm.at[:, my_cols], top, local_sem.at[1])
    load_w.start()
    load_top.start()

    barrier = pltpu.get_barrier_semaphore()
    for k in range(1, m):
        pl.semaphore_signal(barrier, inc=1, device_id={"mp": lax.rem(me + k, m)}, device_id_type=MESH)
    pl.semaphore_signal(barrier, inc=1, device_id={"section": 1 - sec}, device_id_type=MESH)

    @pl.when(r > 0)
    def _():
        pl.semaphore_signal(barrier, inc=1, device_id={"dp": r - 1}, device_id_type=MESH)

    @pl.when(r < n - 1)
    def _():
        pl.semaphore_signal(barrier, inc=1, device_id={"dp": r + 1}, device_id_type=MESH)

    lane = lambda rows: lax.broadcasted_iota(jnp.int32, (rows, 128), 1)

    def norm_tile(i, _):
        rows = pl.ds(pl.multiple_of(i * 16, 16), 16)
        values = x[rows, :].astype(F32)
        average = jnp.sum(values, axis=-1, keepdims=True) * (1.0 / width)
        centred = values - average
        variance = jnp.sum(centred * centred, axis=-1, keepdims=True) * (1.0 / width)
        inv = lax.rsqrt(variance + 1e-06)
        normed[rows, :] = (centred * inv * gain[...]).astype(BF16)
        stats[rows, :] = jnp.where(lane(16) == 0, average, inv)
        return 0

    lax.fori_loop(0, tokens // 16, norm_tile, 0, unroll=2)

    features = vg.shape[1]
    vgt[...] = (vg[...].T * live[...]).reshape(n, features // n, tokens)

    pl.semaphore_wait(barrier, m + jnp.where(r > 0, 1, 0) + jnp.where(r < n - 1, 1, 0))

    def right_copy(c, b, source):
        return pltpu.make_async_remote_copy(
            src_ref=source.at[c, b], dst_ref=from_left.at[c, b], send_sem=right_send.at[c, b],
            recv_sem=right_recv.at[c, b], device_id={"dp": lax.rem(r + 1, n)}, device_id_type=MESH,
        )

    def left_copy(c, b, source):
        return pltpu.make_async_remote_copy(
            src_ref=source.at[c, b], dst_ref=from_right.at[c, b], send_sem=left_send.at[c, b],
            recv_sem=left_recv.at[c, b], device_id={"dp": lax.rem(r + n - 1, n)}, device_id_type=MESH,
        )

    def product(c):
        def block(i, _):
            b = jnp.where(r == 0, n - 1 - i, i)
            own[c, b] = jnp.dot(
                vgt[b], normed[:, c * CHUNK:(c + 1) * CHUNK], preferred_element_type=F32
            ).astype(BF16)

            @pl.when((r == 0) & (b > 0))
            def _():
                right_copy(c, b, own).start()

            @pl.when((r == n - 1) & (b < n - 1))
            def _():
                left_copy(c, b, own).start()

            return 0

        lax.fori_loop(0, n, block, 0)

    def peer(k):
        return {"mp": lax.rem(me + k, m)}

    def part_copy(k):
        return pltpu.make_async_remote_copy(
            src_ref=psend.at[k], dst_ref=precv.at[k], send_sem=p_send.at[k], recv_sem=p_recv.at[k],
            device_id=peer(k), device_id_type=MESH,
        )

    def sum_copy(k):
        return pltpu.make_async_remote_copy(
            src_ref=ssend, dst_ref=srecv.at[k], send_sem=s_send.at[k], recv_sem=s_recv.at[k],
            device_id=peer(k), device_id_type=MESH,
        )

    def fold(value):
        total = value[:, :128]
        for start in range(128, value.shape[1], 128):
            total = total + value[:, start:start + 128]
        return total

    def whitened_of(rows, cols):
        return (x[rows, cols].astype(F32) - stats[rows, 0:1]) * stats[rows, 1:2]

    def partials():
        load_w.wait()
        for step in range(m):
            k = (step + 1) % m
            cols = pl.ds(pl.multiple_of(lax.rem(me + k, m) * share, 128), share)

            def tile(i, _):
                rows = pl.ds(pl.multiple_of(i * rows_mp, rows_mp), rows_mp)
                part = jnp.dot(vg[rows, :], w[:, cols], preferred_element_type=F32)
                psend[k, rows, :] = part.astype(BF16)
                scaled = part * gain[:, cols]
                first, second = fold(scaled), fold(scaled * whitened_of(rows, cols))
                if step == 0:
                    acc1[rows, :] = first
                    acc2[rows, :] = second
                elif step < m - 1:
                    acc1[rows, :] += first
                    acc2[rows, :] += second
                else:
                    one = jnp.sum(acc1[rows, :] + first, axis=-1, keepdims=True)
                    two = jnp.sum(acc2[rows, :] + second, axis=-1, keepdims=True)
                    ssend[rows, :] = jnp.where(lane(rows_mp) == 0, one, two)
                return 0

            lax.fori_loop(0, tokens // rows_mp, tile, 0)
            if k > 0:
                part_copy(k).start()
        for k in range(1, m):
            sum_copy(k).start()

    def section_copy():
        return pltpu.make_async_remote_copy(
            src_ref=above, dst_ref=below, send_sem=sec_send, recv_sem=sec_recv,
            device_id={"section": 1 - sec}, device_id_type=MESH,
        )

    def residual(base, extra):
        def tile(i, _):
            rows = pl.ds(pl.multiple_of(i * 64, 64), 64)
            grad = psend[0, rows, :].astype(F32)
            sums = ssend[rows, :]
            for k in range(1, m):
                grad = grad + precv[k, rows, :].astype(F32)
                sums = sums + srecv[k, rows, :]
            sums = sums * (1.0 / width)
            scaled = grad * gain[:, my_cols]
            white = whitened_of(rows, my_cols)
            branch = stats[rows, 1:2] * (scaled - sums[:, 0:1] - white * sums[:, 1:2])
            value = (base[rows, :].astype(F32) + branch).astype(BF16)
            res[rows, :] = value
            if extra is not None:
                extra[rows, :] = value
            return 0

        lax.fori_loop(0, tokens // 64, tile, 0)

    def finish_later():
        load_top.wait()
        for k in range(1, m):
            part_copy(k).wait_recv()
            sum_copy(k).wait_recv()

        @pl.when(sec == 1)
        def _():
            residual(top, above)
            section_copy().start()

    def finish_earlier():
        @pl.when(sec == 0)
        def _():
            section_copy().wait_recv()
            residual(below, None)

    def forward(c):
        middle = (r > 0) & (r < n - 1)

        def go_right(i, _):
            b = n - 1 - i
            right_copy(c, b, from_left).wait_recv()
            from_left[c, b] = (from_left[c, b].astype(F32) + own[c, b].astype(F32)).astype(BF16)
            right_copy(c, b, from_left).start()
            return 0

        def go_left(b, _):
            left_copy(c, b, from_right).wait_recv()
            from_right[c, b] = (from_right[c, b].astype(F32) + own[c, b].astype(F32)).astype(BF16)
            left_copy(c, b, from_right).start()
            return 0

        def both(right_first):
            steps = [
                lambda: lax.fori_loop(0, n - 1 - r, go_right, 0),
                lambda: lax.fori_loop(0, r, go_left, 0),
            ]
            for step in steps if right_first else steps[::-1]:
                step()

        @pl.when(middle & (r < n // 2))
        def _():
            both(True)

        @pl.when(middle & (r >= n // 2))
        def _():
            both(False)

    def settle(c):
        cols = slice(c * CHUNK, (c + 1) * CHUNK)

        @pl.when(r == 0)
        def _():
            left_copy(c, r, own).wait_recv()
            wg[:, cols] = (own[c, r].astype(F32) + from_right[c, r].astype(F32)).astype(BF16)

        @pl.when(r == n - 1)
        def _():
            right_copy(c, r, own).wait_recv()
            wg[:, cols] = (own[c, r].astype(F32) + from_left[c, r].astype(F32)).astype(BF16)

        @pl.when((r > 0) & (r < n - 1))
        def _():
            left_copy(c, r, own).wait_recv()
            right_copy(c, r, own).wait_recv()
            wg[:, cols] = (
                own[c, r].astype(F32) + from_left[c, r].astype(F32) + from_right[c, r].astype(F32)
            ).astype(BF16)

    product(0)
    partials()
    for c in range(1, chunks):
        product(c)
    later, earlier = max(chunks - 3, 0), max(chunks - 2, 0)
    for c in range(chunks):
        forward(c)
        settle(c)
        if c == later:
            finish_later()
        if c == earlier:
            finish_earlier()

    for k in range(1, m):
        part_copy(k).wait_send()
        sum_copy(k).wait_send()

    @pl.when(sec == 1)
    def _():
        section_copy().wait_send()

    for c in range(chunks):
        def sent_right(b, _):
            right_copy(c, b, own).wait_send()
            return 0

        def sent_left(b, _):
            left_copy(c, b, own).wait_send()
            return 0

        lax.fori_loop(r + 1, n, sent_right, 0)
        lax.fori_loop(0, r, sent_left, 0)


def pass_kernel(wg_in, res_in, wg_out, res_out):
    wg_out[...] = wg_in[...]
    res_out[...] = res_in[...]


def passed_on(wg, res):
    steps = 4
    specs = [
        pl.BlockSpec((wg.shape[0], wg.shape[1] // steps), lambda i: (0, i)),
        pl.BlockSpec((res.shape[0] // steps, res.shape[1]), lambda i: (i, 0)),
    ]
    return pl.pallas_call(
        pass_kernel,
        grid=(steps,),
        out_shape=(jax.ShapeDtypeStruct(wg.shape, wg.dtype), jax.ShapeDtypeStruct(res.shape, res.dtype)),
        in_specs=specs,
        out_specs=tuple(specs),
        compiler_params=pltpu.CompilerParams(vmem_limit_bytes=8 * 2**20),
    )(wg, res)


def solution(mesh):
    n, m = mesh.shape["dp"], mesh.shape["mp"]

    def step(value_grad, stream, weights, gain, top_grad, counts):
        tokens, features = value_grad.shape[1:]
        width = stream.shape[2]
        share, block, chunks = width // m, features // n, width // CHUNK
        micro = jnp.arange(tokens, dtype=jnp.int32) // TOK_MB
        live = (micro < counts[0]).astype(BF16)
        vmem = pl.BlockSpec(memory_space=pltpu.VMEM)
        hbm = pl.BlockSpec(memory_space=pl.ANY)
        dma = pltpu.SemaphoreType.DMA
        chain = (chunks, n, block, CHUNK)
        wg, res = pl.pallas_call(
            functools.partial(kernel, n, m),
            out_shape=(
                jax.ShapeDtypeStruct((block, width), BF16),
                jax.ShapeDtypeStruct((tokens, share), BF16),
            ),
            in_specs=[vmem, vmem, vmem, hbm, vmem, hbm],
            out_specs=(vmem, vmem),
            scratch_shapes=[
                pltpu.VMEM((features, width), BF16),
                pltpu.VMEM((tokens, share), BF16),
                pltpu.VMEM((n, block, tokens), BF16),
                pltpu.VMEM((tokens, width), BF16),
                pltpu.VMEM((tokens, 128), F32),
                pltpu.VMEM(chain, BF16),
                pltpu.VMEM(chain, BF16),
                pltpu.VMEM(chain, BF16),
                pltpu.VMEM((m, tokens, share), BF16),
                pltpu.VMEM((m, tokens, share), BF16),
                pltpu.VMEM((tokens, 128), F32),
                pltpu.VMEM((tokens, 128), F32),
                pltpu.VMEM((tokens, 128), F32),
                pltpu.VMEM((m, tokens, 128), F32),
                pltpu.VMEM((tokens, share), BF16),
                pltpu.VMEM((tokens, share), BF16),
                dma((2,)),
                dma((chunks, n)), dma((chunks, n)), dma((chunks, n)), dma((chunks, n)),
                dma((m,)), dma((m,)), dma((m,)), dma((m,)),
                dma, dma,
            ],
            compiler_params=pltpu.CompilerParams(
                collective_id=0, has_side_effects=True, vmem_limit_bytes=46 * 2**20
            ),
        )(live[None, :], value_grad[0], stream[0], weights[0], gain, top_grad)
        return tuple(a[None] for a in passed_on(wg, res))

    in_specs = (
        P("section", "dp", "mp"),
        P("section", "dp", None),
        P("section", "mp", None),
        P("section", None),
        P("dp", None),
        P("dp"),
    )
    out_specs = (P("section", ("mp", "dp"), None), P("section", "dp", "mp"))
    return jax.shard_map(step, mesh=mesh, in_specs=in_specs, out_specs=out_specs, check_vma=False)
```

```python
import functools

import jax
import jax.numpy as jnp
from jax import lax
from jax.experimental import pallas as pl
from jax.experimental.pallas import tpu as pltpu
from jax.sharding import PartitionSpec as P

MESH = pl.DeviceIdType.MESH
TOK_MB = 256
CHUNK = 512
PIECES = 4
F32, BF16 = jnp.float32, jnp.bfloat16


def kernel(
    n, m, live, vg_hbm, x_hbm, w_hbm, gain_hbm, top_hbm, wg, res,
    vg, x, gain, w, top, vgt, normed, stats, own, from_left, from_right, psend, precv, acc1, acc2, ssend, srecv, above, below,
    local_sem, right_send, right_recv, left_send, left_recv, p_send, p_recv, s_send, s_recv, sec_send, sec_recv,
):
    sec, me, r = lax.axis_index("section"), lax.axis_index("mp"), lax.axis_index("dp")
    tokens, width = x.shape
    share = width // m
    chunks = width // CHUNK
    rows_mp = min(128, tokens)
    my_cols = pl.ds(pl.multiple_of(me * share, 128), share)

    load_w = pltpu.make_async_copy(w_hbm, w, local_sem.at[0])
    load_top = pltpu.make_async_copy(top_hbm.at[:, my_cols], top, local_sem.at[1])
    load_gain = pltpu.make_async_copy(gain_hbm, gain, local_sem.at[2])
    load_vg = pltpu.make_async_copy(vg_hbm, vg, local_sem.at[3])
    piece = tokens // PIECES

    def load_x(p):
        rows = pl.ds(p * piece, piece)
        return pltpu.make_async_copy(x_hbm.at[rows, :], x.at[rows, :], local_sem.at[4 + p])

    load_gain.start()
    for p in range(PIECES):
        load_x(p).start()
    load_vg.start()
    load_w.start()
    load_top.start()

    barrier = pltpu.get_barrier_semaphore()
    for k in range(1, m):
        pl.semaphore_signal(barrier, inc=1, device_id={"mp": lax.rem(me + k, m)}, device_id_type=MESH)
    pl.semaphore_signal(barrier, inc=1, device_id={"section": 1 - sec}, device_id_type=MESH)

    @pl.when(r > 0)
    def _():
        pl.semaphore_signal(barrier, inc=1, device_id={"dp": r - 1}, device_id_type=MESH)

    @pl.when(r < n - 1)
    def _():
        pl.semaphore_signal(barrier, inc=1, device_id={"dp": r + 1}, device_id_type=MESH)

    lane = lambda rows: lax.broadcasted_iota(jnp.int32, (rows, 128), 1)

    def norm_tile(i, _):
        rows = pl.ds(pl.multiple_of(i * 16, 16), 16)
        values = x[rows, :].astype(F32)
        average = jnp.sum(values, axis=-1, keepdims=True) * (1.0 / width)
        centred = values - average
        variance = jnp.sum(centred * centred, axis=-1, keepdims=True) * (1.0 / width)
        inv = lax.rsqrt(variance + 1e-06)
        normed[rows, :] = (centred * inv * gain[...]).astype(BF16)
        stats[rows, :] = jnp.where(lane(16) == 0, average, inv)
        return 0

    load_gain.wait()
    for p in range(PIECES):
        load_x(p).wait()
        lax.fori_loop(p * (piece // 16), (p + 1) * (piece // 16), norm_tile, 0, unroll=2)
    load_vg.wait()

    features = vg.shape[1]
    vgt[...] = (vg[...].T * live[...]).reshape(n, features // n, tokens)

    pl.semaphore_wait(barrier, m + jnp.where(r > 0, 1, 0) + jnp.where(r < n - 1, 1, 0))

    def right_copy(c, b, source):
        return pltpu.make_async_remote_copy(
            src_ref=source.at[c, b], dst_ref=from_left.at[c, b], send_sem=right_send.at[c, b],
            recv_sem=right_recv.at[c, b], device_id={"dp": lax.rem(r + 1, n)}, device_id_type=MESH,
        )

    def left_copy(c, b, source):
        return pltpu.make_async_remote_copy(
            src_ref=source.at[c, b], dst_ref=from_right.at[c, b], send_sem=left_send.at[c, b],
            recv_sem=left_recv.at[c, b], device_id={"dp": lax.rem(r + n - 1, n)}, device_id_type=MESH,
        )

    def product(c):
        def block(i, _):
            b = jnp.where(r == 0, n - 1 - i, i)
            own[c, b] = jnp.dot(
                vgt[b], normed[:, c * CHUNK:(c + 1) * CHUNK], preferred_element_type=F32
            ).astype(BF16)

            @pl.when((r == 0) & (b > 0))
            def _():
                right_copy(c, b, own).start()

            @pl.when((r == n - 1) & (b < n - 1))
            def _():
                left_copy(c, b, own).start()

            return 0

        lax.fori_loop(0, n, block, 0)

    def peer(k):
        return {"mp": lax.rem(me + k, m)}

    def part_copy(k):
        return pltpu.make_async_remote_copy(
            src_ref=psend.at[k], dst_ref=precv.at[k], send_sem=p_send.at[k], recv_sem=p_recv.at[k],
            device_id=peer(k), device_id_type=MESH,
        )

    def sum_copy(k):
        return pltpu.make_async_remote_copy(
            src_ref=ssend, dst_ref=srecv.at[k], send_sem=s_send.at[k], recv_sem=s_recv.at[k],
            device_id=peer(k), device_id_type=MESH,
        )

    def fold(value):
        total = value[:, :128]
        for start in range(128, value.shape[1], 128):
            total = total + value[:, start:start + 128]
        return total

    def whitened_of(rows, cols):
        return (x[rows, cols].astype(F32) - stats[rows, 0:1]) * stats[rows, 1:2]

    def partials():
        load_w.wait()
        for step in range(m):
            k = (step + 1) % m
            cols = pl.ds(pl.multiple_of(lax.rem(me + k, m) * share, 128), share)

            def tile(i, _):
                rows = pl.ds(pl.multiple_of(i * rows_mp, rows_mp), rows_mp)
                part = jnp.dot(vg[rows, :], w[:, cols], preferred_element_type=F32)
                psend[k, rows, :] = part.astype(BF16)
                scaled = part * gain[:, cols]
                first, second = fold(scaled), fold(scaled * whitened_of(rows, cols))
                if step == 0:
                    acc1[rows, :] = first
                    acc2[rows, :] = second
                elif step < m - 1:
                    acc1[rows, :] += first
                    acc2[rows, :] += second
                else:
                    one = jnp.sum(acc1[rows, :] + first, axis=-1, keepdims=True)
                    two = jnp.sum(acc2[rows, :] + second, axis=-1, keepdims=True)
                    ssend[rows, :] = jnp.where(lane(rows_mp) == 0, one, two)
                return 0

            lax.fori_loop(0, tokens // rows_mp, tile, 0)
            if k > 0:
                part_copy(k).start()
        for k in range(1, m):
            sum_copy(k).start()

    def section_copy():
        return pltpu.make_async_remote_copy(
            src_ref=above, dst_ref=below, send_sem=sec_send, recv_sem=sec_recv,
            device_id={"section": 1 - sec}, device_id_type=MESH,
        )

    def residual(base, extra):
        def tile(i, _):
            rows = pl.ds(pl.multiple_of(i * 64, 64), 64)
            grad = psend[0, rows, :].astype(F32)
            sums = ssend[rows, :]
            for k in range(1, m):
                grad = grad + precv[k, rows, :].astype(F32)
                sums = sums + srecv[k, rows, :]
            sums = sums * (1.0 / width)
            scaled = grad * gain[:, my_cols]
            white = whitened_of(rows, my_cols)
            branch = stats[rows, 1:2] * (scaled - sums[:, 0:1] - white * sums[:, 1:2])
            value = (base[rows, :].astype(F32) + branch).astype(BF16)
            res[rows, :] = value
            if extra is not None:
                extra[rows, :] = value
            return 0

        lax.fori_loop(0, tokens // 64, tile, 0)

    def finish_later():
        load_top.wait()
        for k in range(1, m):
            part_copy(k).wait_recv()
            sum_copy(k).wait_recv()

        @pl.when(sec == 1)
        def _():
            residual(top, above)
            section_copy().start()

    def finish_earlier():
        @pl.when(sec == 0)
        def _():
            section_copy().wait_recv()
            residual(below, None)

    def forward(c):
        middle = (r > 0) & (r < n - 1)

        def go_right(i, _):
            b = n - 1 - i
            right_copy(c, b, from_left).wait_recv()
            from_left[c, b] = (from_left[c, b].astype(F32) + own[c, b].astype(F32)).astype(BF16)
            right_copy(c, b, from_left).start()
            return 0

        def go_left(b, _):
            left_copy(c, b, from_right).wait_recv()
            from_right[c, b] = (from_right[c, b].astype(F32) + own[c, b].astype(F32)).astype(BF16)
            left_copy(c, b, from_right).start()
            return 0

        def both(right_first):
            steps = [
                lambda: lax.fori_loop(0, n - 1 - r, go_right, 0),
                lambda: lax.fori_loop(0, r, go_left, 0),
            ]
            for step in steps if right_first else steps[::-1]:
                step()

        @pl.when(middle & (r < n // 2))
        def _():
            both(True)

        @pl.when(middle & (r >= n // 2))
        def _():
            both(False)

    def settle(c):
        cols = slice(c * CHUNK, (c + 1) * CHUNK)

        @pl.when(r == 0)
        def _():
            left_copy(c, r, own).wait_recv()
            wg[:, cols] = (own[c, r].astype(F32) + from_right[c, r].astype(F32)).astype(BF16)

        @pl.when(r == n - 1)
        def _():
            right_copy(c, r, own).wait_recv()
            wg[:, cols] = (own[c, r].astype(F32) + from_left[c, r].astype(F32)).astype(BF16)

        @pl.when((r > 0) & (r < n - 1))
        def _():
            left_copy(c, r, own).wait_recv()
            right_copy(c, r, own).wait_recv()
            wg[:, cols] = (
                own[c, r].astype(F32) + from_left[c, r].astype(F32) + from_right[c, r].astype(F32)
            ).astype(BF16)

    product(0)
    partials()
    for c in range(1, chunks):
        product(c)
    later, earlier = max(chunks - 3, 0), max(chunks - 2, 0)
    for c in range(chunks):
        forward(c)
        settle(c)
        if c == later:
            finish_later()
        if c == earlier:
            finish_earlier()

    for k in range(1, m):
        part_copy(k).wait_send()
        sum_copy(k).wait_send()

    @pl.when(sec == 1)
    def _():
        section_copy().wait_send()

    for c in range(chunks):
        def sent_right(b, _):
            right_copy(c, b, own).wait_send()
            return 0

        def sent_left(b, _):
            left_copy(c, b, own).wait_send()
            return 0

        lax.fori_loop(r + 1, n, sent_right, 0)
        lax.fori_loop(0, r, sent_left, 0)


def pass_kernel(wg_in, res_in, wg_out, res_out):
    wg_out[...] = wg_in[...]
    res_out[...] = res_in[...]


def passed_on(wg, res):
    steps = 4
    specs = [
        pl.BlockSpec((wg.shape[0], wg.shape[1] // steps), lambda i: (0, i)),
        pl.BlockSpec((res.shape[0] // steps, res.shape[1]), lambda i: (i, 0)),
    ]
    return pl.pallas_call(
        pass_kernel,
        grid=(steps,),
        out_shape=(jax.ShapeDtypeStruct(wg.shape, wg.dtype), jax.ShapeDtypeStruct(res.shape, res.dtype)),
        in_specs=specs,
        out_specs=tuple(specs),
        compiler_params=pltpu.CompilerParams(vmem_limit_bytes=60 * 2**20),
    )(wg, res)


def solution(mesh):
    n, m = mesh.shape["dp"], mesh.shape["mp"]

    def step(value_grad, stream, weights, gain, top_grad, counts):
        tokens, features = value_grad.shape[1:]
        width = stream.shape[2]
        share, block, chunks = width // m, features // n, width // CHUNK
        micro = jnp.arange(tokens, dtype=jnp.int32) // TOK_MB
        live = (micro < counts[0]).astype(BF16)
        vmem = pl.BlockSpec(memory_space=pltpu.VMEM)
        hbm = pl.BlockSpec(memory_space=pltpu.HBM)
        dma = pltpu.SemaphoreType.DMA
        chain = (chunks, n, block, CHUNK)
        wg, res = pl.pallas_call(
            functools.partial(kernel, n, m),
            out_shape=(
                jax.ShapeDtypeStruct((block, width), BF16),
                jax.ShapeDtypeStruct((tokens, share), BF16),
            ),
            in_specs=[vmem, hbm, hbm, hbm, hbm, hbm],
            out_specs=(vmem, vmem),
            scratch_shapes=[
                pltpu.VMEM((tokens, features), BF16),
                pltpu.VMEM((tokens, width), BF16),
                pltpu.VMEM((1, width), F32),
                pltpu.VMEM((features, width), BF16),
                pltpu.VMEM((tokens, share), BF16),
                pltpu.VMEM((n, block, tokens), BF16),
                pltpu.VMEM((tokens, width), BF16),
                pltpu.VMEM((tokens, 128), F32),
                pltpu.VMEM(chain, BF16),
                pltpu.VMEM(chain, BF16),
                pltpu.VMEM(chain, BF16),
                pltpu.VMEM((m, tokens, share), BF16),
                pltpu.VMEM((m, tokens, share), BF16),
                pltpu.VMEM((tokens, 128), F32),
                pltpu.VMEM((tokens, 128), F32),
                pltpu.VMEM((tokens, 128), F32),
                pltpu.VMEM((m, tokens, 128), F32),
                pltpu.VMEM((tokens, share), BF16),
                pltpu.VMEM((tokens, share), BF16),
                dma((4 + PIECES,)),
                dma((chunks, n)), dma((chunks, n)), dma((chunks, n)), dma((chunks, n)),
                dma((m,)), dma((m,)), dma((m,)), dma((m,)),
                dma, dma,
            ],
            compiler_params=pltpu.CompilerParams(
                collective_id=0, has_side_effects=True, vmem_limit_bytes=60 * 2**20
            ),
        )(live[None, :], value_grad[0], stream[0], weights[0], gain, top_grad)
        return tuple(a[None] for a in passed_on(wg, res))

    in_specs = (
        P("section", "dp", "mp"),
        P("section", "dp", None),
        P("section", "mp", None),
        P("section", None),
        P("dp", None),
        P("dp"),
    )
    out_specs = (P("section", ("mp", "dp"), None), P("section", "dp", "mp"))
    return jax.shard_map(step, mesh=mesh, in_specs=in_specs, out_specs=out_specs, check_vma=False)
```
